256 devices in a mesh: gx: 4 (over y), gy: 16 (over z, core), gz: 4 (over x).
Axes of the slice: x: 4, y: 4, z: 8, core: 2. Of those that a mesh axis runs over, the one named last changes fastest.
Arguments:
- pair: bfloat16 [128, 1024, 1024], P('gz', 'gy', 'gx'), may hold values from -6 to 6
- pair_mask: int32 [1024, 1024], P('gy', 'gx'), may hold values 0 or 1
- in_gain: float32 [128], replicated, may hold values from 0.5 to 2
- w_left: bfloat16 [128, 128], P(None, 'gz'), may hold values from -0.5 to 0.5
- w_left_gate: bfloat16 [128, 128], P(None, 'gz'), may hold values from -0.5 to 0.5
- w_right: bfloat16 [128, 128], P(None, 'gz'), may hold values from -0.5 to 0.5
- w_right_gate: bfloat16 [128, 128], P(None, 'gz'), may hold values from -0.5 to 0.5
- w_out_gate: bfloat16 [128, 128], P(None, 'gz'), may hold values from -0.5 to 0.5
- out_gain: float32 [128], P('gz'), may hold values from 0.5 to 2
- w_out: bfloat16 [128, 128], P(None, 'gz'), may hold values from -0.5 to 0.5
Outputs:
- update: bfloat16 [128, 1024, 1024], P('gz', 'gy', 'gx')
The draws below stay inside these ranges and needn't reach their ends.
All inputs are finite; a program needn't handle non-finite values. No bound on the sum of `pair_mask` on one device may be relied on, other than what follows from the above.
Results may differ from the reference program's by a relative error of at most 0.0078.
Values may be sent and summed in bfloat16 or wider, within the bound.
A program may use at most 128 MiB of HBM per device.

```python
import math
import jax
import jax.numpy as jnp
from jax import lax

CZ = 128
CH = 128
N = 1024


def set_ends(values, own_key, smallest, high):
    longest = values.shape.index(max(values.shape))
    spots = []
    for shift in (0, 1):
        where = [jax.random.randint(jax.random.fold_in(own_key, axis), (), 0, length) for axis, length in enumerate(values.shape)]
        where[longest] = (where[longest] + shift) % values.shape[longest]
        spots.append(tuple(where))
    return values.at[spots[0]].set(smallest).at[spots[1]].set(high)


def block_levels(own_key, shape, shards, least, top_value):
    level, own = 1.0, jax.random.fold_in(own_key, 6)
    for dim, shards_of in shards:
        steps = jnp.exp(jax.random.uniform(jax.random.fold_in(own, dim), (shards_of,), jnp.float32, least / len(shards), top_value / len(shards)))
        level = level * jnp.repeat(steps, shape[dim] // shards_of).reshape([-1 if axis == dim else 1 for axis in range(len(shape))])
    return level


def normal_values(key, dims, deviation, bound, cuts=(), held_as=jnp.bfloat16):
    entries = jax.random.normal(key, dims, jnp.float32) * deviation
    if len(cuts) > 0:
        entries = block_levels(key, dims, cuts, -0.22, 0.18) * entries
    return jnp.clip(entries, min=-bound, max=bound).astype(held_as)


def setup_inputs(seed: int = 0) -> dict:
    arg_keys = jax.random.split(jax.random.key(seed), 11)
    pair = normal_values(arg_keys[0], (CZ, N, N), 1.0, 6.0, ((0, 4), (1, 16), (2, 4)))
    pair_mask = set_ends((jax.random.randint(arg_keys[1], (N, N), 0, 8) < 7).astype(jnp.int32), jax.random.fold_in(arg_keys[1], 1), 0, 1)
    in_gain = jnp.clip(jnp.exp(jax.random.uniform(arg_keys[2], (CZ,), jnp.float32, math.log(0.5), math.log(2.0))), 0.5, 2.0)
    w_left = normal_values(arg_keys[3], (CZ, CH), CZ ** -0.5, 0.5, ((1, 4),))
    w_left_gate = normal_values(arg_keys[4], (CZ, CH), CZ ** -0.5, 0.5, ((1, 4),))
    w_right = normal_values(arg_keys[5], (CZ, CH), CZ ** -0.5, 0.5, ((1, 4),))
    w_right_gate = normal_values(arg_keys[6], (CZ, CH), CZ ** -0.5, 0.5, ((1, 4),))
    w_out_gate = normal_values(arg_keys[7], (CZ, CZ), CZ ** -0.5, 0.5, ((1, 4),))
    out_gain = jnp.clip(jnp.exp(math.log(2.0) - 1.3862944 * jax.random.uniform(arg_keys[8], (CH,), jnp.float32) ** block_levels(arg_keys[8], (CH,), ((0, 4),), -0.2, 0.2)), 0.5, 2.0)
    w_out = normal_values(arg_keys[9], (CH, CZ), CH ** -0.5, 0.5, ((1, 4),))
    return {"pair": pair, "pair_mask": pair_mask, "in_gain": in_gain, "w_left": w_left, "w_left_gate": w_left_gate, "w_right": w_right, "w_right_gate": w_right_gate, "w_out_gate": w_out_gate, "out_gain": out_gain, "w_out": w_out}


epsilon = 1e-05

def layer_norm(values, gain):
    average = lax.optimization_barrier(jnp.mean(values, axis=0))
    centered = values - average
    spread = lax.optimization_barrier(jnp.mean(jnp.square(centered), axis=0))
    return centered * lax.rsqrt(spread + epsilon) * gain[:, None, None]

def reference(pair, pair_mask, in_gain, w_left, w_left_gate, w_right, w_right_gate, w_out_gate, out_gain, w_out):
    normed = layer_norm(pair.astype(jnp.float32), in_gain).astype(jnp.bfloat16)
    normed_f = normed.astype(jnp.float32)
    mask_float = pair_mask.astype(jnp.float32)[None]

    def project(weight):
        return jnp.einsum('cik,ch->hik', normed_f, weight.astype(jnp.float32))
    left_rows = (mask_float * jax.nn.sigmoid(project(w_left_gate)) * project(w_left)).astype(jnp.bfloat16)
    right_rows = (mask_float * jax.nn.sigmoid(project(w_right_gate)) * project(w_right)).astype(jnp.bfloat16)

    def channel_product(operands):
        return jnp.dot(operands[0], operands[1].T, preferred_element_type=jnp.float32)
    mixed_sum = lax.map(channel_product, (left_rows, right_rows))
    normed_mix = layer_norm(mixed_sum, out_gain).astype(jnp.bfloat16)
    out_gate = jax.nn.sigmoid(jnp.einsum('cij,cd->dij', normed_f, w_out_gate.astype(jnp.float32)))
    projected = jnp.einsum('hij,hd->dij', normed_mix.astype(jnp.float32), w_out.astype(jnp.float32))
    return (out_gate * projected).astype(jnp.bfloat16)
```

```python
import jax
import jax.numpy as jnp
from jax import lax
from jax.experimental import pallas as pl
from jax.experimental.pallas import tpu as pltpu
from jax.sharding import PartitionSpec as P

epsilon = 1e-05
MESH = pl.DeviceIdType.MESH
F32 = jnp.float32
BF16 = jnp.bfloat16


def offset(i):
    return lax.rem(i, 4), lax.rem(i // 4 + i, 4), lax.rem(i // 16 + i, 8)


def kernel(
    pair_ref, mask_ref, gain_ref, weights_ref, out_gain_ref, out_ref,
    pair_rows, x, weights, out_gain, mask, staged, to_heads, gate, held, product, mixed, update, out_rows,
    row_send, row_recv, weight_send, weight_recv, gain_send, gain_recv,
    head_send, head_recv, core_send, core_recv, mix_send, mix_recv, up_send, up_recv,
):
    gx, gy, gz = lax.axis_index("gx"), lax.axis_index("gy"), lax.axis_index("gz")
    z, core = gy // 2, lax.rem(gy, 2)
    head = (gz * 4 + gx) * 8 + z
    mine = pl.ds(pl.multiple_of(gz * 32, 32), 32)

    def chip(i):
        dx, dy, dz = offset(i)
        return lax.rem(gz + dx, 4), lax.rem(gx + dy, 4), lax.rem(z + dz, 8)

    def source(i):
        dx, dy, dz = offset(i)
        return lax.rem(gz - dx + 4, 4), lax.rem(gx - dy + 4, 4), lax.rem(z - dz + 8, 8)

    def device(px, py, pz):
        return {"gx": py, "gy": pz * 2 + core, "gz": px}

    def beside(d):
        return lax.rem(gz + d, 4)

    barrier = pltpu.get_barrier_semaphore()

    def greet(i, carry):
        pl.semaphore_signal(barrier, inc=1, device_id=device(*chip(i)), device_id_type=MESH)
        return carry

    lax.fori_loop(1, 128, greet, 0)
    pl.semaphore_signal(barrier, inc=1, device_id={"gy": z * 2 + 1 - core}, device_id_type=MESH)

    for c0 in range(0, 32, 16):
        for i0 in range(0, 64, 16):
            pair_rows[i0 : i0 + 16, c0 : c0 + 16, :] = jnp.swapaxes(
                pair_ref[c0 : c0 + 16, i0 : i0 + 16, :], 0, 1
            )
    mask[...] = mask_ref[pl.ds(pl.multiple_of(gz * 16, 16), 16), :].astype(F32)
    pl.semaphore_wait(barrier, 128)

    def weight_copy(d):
        return pltpu.make_async_remote_copy(
            weights_ref, weights.at[:, mine, :], weight_send.at[d], weight_recv.at[d],
            device_id={"gz": beside(d)}, device_id_type=MESH,
        )

    def gain_copy(d):
        return pltpu.make_async_remote_copy(
            out_gain_ref, out_gain.at[mine, :], gain_send.at[d], gain_recv.at[d],
            device_id={"gz": beside(d)}, device_id_type=MESH,
        )

    def row_copy(d, n):
        return pltpu.make_async_remote_copy(
            pair_rows.at[pl.ds(beside(d) * 16 + n * 4, 4)], x.at[n * 4 : n * 4 + 4, mine, :],
            row_send.at[d, n], row_recv.at[d, n], device_id={"gz": beside(d)}, device_id_type=MESH,
        )

    for d in (1, 3, 2):
        weight_copy(d).start()
    for n in range(4):
        for d in (1, 3, 2):
            row_copy(d, n).start()
    for d in (1, 3, 2):
        gain_copy(d).start()
    x[:, mine, :] = pair_rows[pl.ds(gz * 16, 16)]
    weights[:, mine, :] = weights_ref[...]
    out_gain[mine, :] = out_gain_ref[...]
    for d in (1, 3, 2):
        weight_copy(d).wait_recv()

    for half in range(2):
        for n in (2 * half, 2 * half + 1):
            for d in (1, 3, 2):
                row_copy(d, n).wait_recv()

            def row(r, carry):
                i = n * 4 + r
                values = x[i].astype(F32)
                average = jnp.mean(values, axis=0, keepdims=True)
                centered = values - average
                spread = jnp.mean(jnp.square(centered), axis=0, keepdims=True)
                normed = (centered * lax.rsqrt(spread + epsilon) * gain_ref[...]).astype(BF16)
                x[i] = normed
                keep = mask[pl.ds(i, 1), :]
                for side in range(2):
                    both = jnp.dot(
                        weights[2 * side : 2 * side + 2].reshape(256, 128), normed,
                        preferred_element_type=F32,
                    )
                    staged[side, i - half * 8] = keep * jax.nn.sigmoid(both[:128]) * both[128:]
                return carry

            lax.fori_loop(0, 4, row, 0)
        for side in range(2):
            for h0 in range(0, 128, 8):
                to_heads[h0 : h0 + 8, side, half * 8 : half * 8 + 8, :] = jnp.swapaxes(
                    staged[side, :, h0 : h0 + 8, :], 0, 1
                ).astype(BF16)

    def place(px, py, pz):
        rows = pl.ds(pl.multiple_of((pz * 2 + core) * 64 + px * 16, 16), 16)
        return rows, pl.ds(pl.multiple_of(py * 256, 256), 256)

    def head_copy(i, at):
        px, py, pz = chip(i)
        rows, columns = place(*at)
        return pltpu.make_async_remote_copy(
            to_heads.at[(px * 4 + py) * 8 + pz], held.at[:, rows, columns],
            head_send.at[i], head_recv.at[i], device_id=device(px, py, pz), device_id_type=MESH,
        )

    def send_head(i, carry):
        head_copy(i, (gz, gx, z)).start()
        return carry

    lax.fori_loop(1, 128, send_head, 0)
    rows, columns = place(gz, gx, z)
    held[:, rows, columns] = to_heads[head]

    def gate_row(i, carry):
        gate[i] = jax.nn.sigmoid(jnp.dot(weights[4], x[i], preferred_element_type=F32))
        return carry

    lax.fori_loop(0, 16, gate_row, 0)

    def take_head(i, carry):
        head_copy(i, source(i)).wait_recv()
        return carry

    lax.fori_loop(1, 128, take_head, 0)

    def core_copy(n, whose):
        part = held.at[1, pl.ds(pl.multiple_of(n * 128 + whose * 64, 64), 64), :]
        return pltpu.make_async_remote_copy(
            part, part, core_send.at[n], core_recv.at[n],
            device_id={"gy": z * 2 + 1 - core}, device_id_type=MESH,
        )

    for n in range(8):
        core_copy(n, core).start()
    for n in range(8):
        core_copy(n, 1 - core).wait_recv()

    for y in range(4):
        right = held[1, y * 256 : y * 256 + 256, :]
        for n in range(8):
            left = held[0, pl.ds(pl.multiple_of(n * 128 + core * 64, 64), 64), :]
            product[y, n * 64 : n * 64 + 64, :] = lax.dot_general(
                left, right, (((1,), (1,)), ((), ())), preferred_element_type=F32
            ).astype(BF16)

    def mix_copy(i, to):
        px, py, pz = chip(i)
        return pltpu.make_async_remote_copy(
            product.at[py, pl.ds(pl.multiple_of(pz * 64 + px * 16, 16), 16), :], mixed.at[to],
            mix_send.at[i], mix_recv.at[i], device_id=device(px, py, pz), device_id_type=MESH,
        )

    def send_mix(i, carry):
        mix_copy(i, head).start()
        return carry

    lax.fori_loop(1, 128, send_mix, 0)
    mixed[head] = product[gx, pl.ds(pl.multiple_of(z * 64 + gz * 16, 16), 16), :]
    for d in (1, 3, 2):
        gain_copy(d).wait_recv()

    def take_mix(i, carry):
        px, py, pz = source(i)
        mix_copy(i, (px * 4 + py) * 8 + pz).wait_recv()
        return carry

    lax.fori_loop(1, 128, take_mix, 0)

    def up_copy(d, n, where):
        theirs = pl.ds(pl.multiple_of(beside(d) * 32, 32), 32)
        return pltpu.make_async_remote_copy(
            update.at[n * 4 : n * 4 + 4, theirs, :], out_rows.at[pl.ds(where * 16 + n * 4, 4)],
            up_send.at[d, n], up_recv.at[d, n], device_id={"gz": beside(d)}, device_id_type=MESH,
        )

    for half in range(2):
        for h0 in range(0, 128, 8):
            staged[0, :, h0 : h0 + 8, :] = jnp.swapaxes(
                mixed[h0 : h0 + 8, half * 8 : half * 8 + 8, :].astype(F32), 0, 1
            )
        for n in (2 * half, 2 * half + 1):

            def last(r, carry):
                i = n * 4 + r
                values = staged[0, i - half * 8]
                average = jnp.mean(values, axis=0, keepdims=True)
                centered = values - average
                spread = jnp.mean(jnp.square(centered), axis=0, keepdims=True)
                normed = (centered * lax.rsqrt(spread + epsilon) * out_gain[...]).astype(BF16)
                projected = jnp.dot(weights[5], normed, preferred_element_type=F32)
                update[i] = (gate[i] * projected).astype(BF16)
                return carry

            lax.fori_loop(0, 4, last, 0)
            for d in (1, 3, 2):
                up_copy(d, n, gz).start()
    out_rows[pl.ds(gz * 16, 16)] = update[:, mine, :]
    for n in range(4):
        for d in (1, 3, 2):
            up_copy(d, n, lax.rem(gz - d + 4, 4)).wait_recv()
    for c0 in range(0, 32, 16):
        for i0 in range(0, 64, 16):
            out_ref[c0 : c0 + 16, i0 : i0 + 16, :] = jnp.swapaxes(
                out_rows[i0 : i0 + 16, c0 : c0 + 16, :], 0, 1
            )

    for d in (1, 3, 2):
        weight_copy(d).wait_send()
        gain_copy(d).wait_send()
        for n in range(4):
            row_copy(d, n).wait_send()
            up_copy(d, n, gz).wait_send()
    for n in range(8):
        core_copy(n, core).wait_send()

    def sent(i, carry):
        head_copy(i, (gz, gx, z)).wait_send()
        mix_copy(i, head).wait_send()
        return carry

    lax.fori_loop(1, 128, sent, 0)


def local(
    pair,
    pair_mask,
    in_gain,
    w_left,
    w_left_gate,
    w_right,
    w_right_gate,
    w_out_gate,
    out_gain,
    w_out,
):
    weights = jnp.stack([w.T for w in (w_left_gate, w_left, w_right_gate, w_right, w_out_gate, w_out)])
    vmem = pl.BlockSpec(memory_space=pltpu.VMEM)
    dma = pltpu.SemaphoreType.DMA
    return pl.pallas_call(
        kernel,
        out_shape=jax.ShapeDtypeStruct((32, 64, 256), BF16),
        in_specs=[vmem] * 5,
        out_specs=vmem,
        scratch_shapes=[
            pltpu.VMEM((64, 32, 256), BF16),
            pltpu.VMEM((16, 128, 256), BF16),
            pltpu.VMEM((6, 128, 128), BF16),
            pltpu.VMEM((128, 256), F32),
            pltpu.VMEM((16, 256), F32),
            pltpu.VMEM((2, 8, 128, 256), F32),
            pltpu.VMEM((128, 2, 16, 256), BF16),
            pltpu.VMEM((16, 128, 256), F32),
            pltpu.VMEM((2, 1024, 1024), BF16),
            pltpu.VMEM((4, 512, 256), BF16),
            pltpu.VMEM((128, 16, 256), BF16),
            pltpu.VMEM((16, 128, 256), BF16),
            pltpu.VMEM((64, 32, 256), BF16),
            dma((4, 4)), dma((4, 4)), dma((4,)), dma((4,)), dma((4,)), dma((4,)),
            dma((128,)), dma((128,)), dma((8,)), dma((8,)), dma((128,)), dma((128,)),
            dma((4, 4)), dma((4, 4)),
        ],
        compiler_params=pltpu.CompilerParams(
            collective_id=0, has_side_effects=True, vmem_limit_bytes=50 * 1024 * 1024
        ),
        name="triangle",
    )(
        pair,
        pair_mask,
        jnp.broadcast_to(in_gain[:, None], (128, 256)),
        weights,
        jnp.broadcast_to(out_gain[:, None], (32, 256)),
    )


def solution(mesh):
    placed = (
        P("gz", "gy", "gx"),
        P("gy", "gx"),
        P(),
        P(None, "gz"),
        P(None, "gz"),
        P(None, "gz"),
        P(None, "gz"),
        P(None, "gz"),
        P("gz"),
        P(None, "gz"),
    )
    return jax.shard_map(
        local, mesh=mesh, in_specs=placed, out_specs=P("gz", "gy", "gx"), check_vma=False
    )
```

```python
import jax
import jax.numpy as jnp
from jax import lax
from jax.experimental import pallas as pl
from jax.experimental.pallas import tpu as pltpu
from jax.sharding import PartitionSpec as P

epsilon = 1e-05
MESH = pl.DeviceIdType.MESH
F32 = jnp.float32
BF16 = jnp.bfloat16


def offset(i):
    return lax.rem(i, 4), lax.rem(i // 4 + i, 4), lax.rem(i // 16 + i, 8)


def column(row):
    return jnp.transpose(jnp.broadcast_to(row, (128, row.shape[1])))


def kernel(
    pair_ref, mask_ref, gain_ref, out_gain_ref, w0, w1, w2, w3, w4, w5, out_ref,
    pair, raw_mask, gain_row, out_gain_row, raw_weights,
    pair_rows, x, weights, gain, out_gain, mask, staged, to_heads, gate, held, total, product, mixed, update,
    load, near, far, row_send, row_recv, weight_send, weight_recv, gain_send, gain_recv,
    head_send, head_recv, core_send, core_recv, mix_send, mix_recv, up_send, up_recv, own,
):
    gx, gy, gz = lax.axis_index("gx"), lax.axis_index("gy"), lax.axis_index("gz")
    z, core = gy // 2, lax.rem(gy, 2)
    head = (gz * 4 + gx) * 8 + z
    mine = pl.ds(pl.multiple_of(gz * 32, 32), 32)
    other = {"gy": z * 2 + 1 - core}

    def chip(i):
        dx, dy, dz = offset(i)
        return lax.rem(gz + dx, 4), lax.rem(gx + dy, 4), lax.rem(z + dz, 8)

    def device(px, py, pz):
        return {"gx": py, "gy": pz * 2 + core, "gz": px}

    def beside(d):
        return lax.rem(gz + d, 4)

    def signal(semaphore, where):
        pl.semaphore_signal(semaphore, inc=1, device_id=where, device_id_type=MESH)

    def along_x(semaphore):
        for d in (1, 3, 2):
            signal(semaphore, {"gz": beside(d)})

    def along_y(semaphore):
        for d in (1, 3, 2):
            signal(semaphore, {"gx": lax.rem(gx + d, 4)})

    def along_z(semaphore):
        for d in (4, 3, 5, 2, 6, 1, 7):
            signal(semaphore, {"gy": lax.rem(z + d, 8) * 2 + core})

    barrier = pltpu.get_barrier_semaphore()
    along_z(barrier)
    along_x(barrier)
    along_y(barrier)
    signal(barrier, other)

    loads = [
        pltpu.make_async_copy(pair_ref, pair, load.at[0]),
        pltpu.make_async_copy(
            mask_ref.at[pl.ds(pl.multiple_of(gz * 16, 16), 16), :], raw_mask, load.at[1]
        ),
        pltpu.make_async_copy(gain_ref, gain_row, load.at[2]),
        pltpu.make_async_copy(out_gain_ref, out_gain_row, load.at[3]),
    ]
    for n, w in enumerate((w0, w1, w2, w3, w4, w5)):
        loads.append(pltpu.make_async_copy(w, raw_weights.at[n], load.at[4 + n]))
    for copy in loads:
        copy.start()
    loads[0].wait()
    for c0 in range(0, 32, 16):
        for i0 in range(0, 64, 16):
            pair_rows[i0 : i0 + 16, c0 : c0 + 16, :] = jnp.swapaxes(
                pair[c0 : c0 + 16, i0 : i0 + 16, :], 0, 1
            )
    for copy in loads[1:]:
        copy.wait()
    for n in range(6):
        weights[n, mine, :] = raw_weights[n]
    for half in range(2):
        for p in range(8):
            pairs = [raw_mask[2 * p + e : 2 * p + e + 1, half * 128 : half * 128 + 128] for e in range(2)]
            mask[half, p] = jnp.concatenate(pairs, axis=1).astype(F32)
    across = column(gain_row[...])
    gain[...] = jnp.concatenate([across, across], axis=1)
    out_gain[mine, :] = column(out_gain_row[...])
    pl.semaphore_wait(barrier, 14)

    def weight_copy(d):
        part = weights.at[:, mine, :]
        return pltpu.make_async_remote_copy(
            part, part, weight_send, weight_recv, device_id={"gz": beside(d)}, device_id_type=MESH
        )

    def gain_copy(d):
        part = out_gain.at[mine, :]
        return pltpu.make_async_remote_copy(
            part, part, gain_send, gain_recv, device_id={"gz": beside(d)}, device_id_type=MESH
        )

    def row_copy(d, half, n):
        return pltpu.make_async_remote_copy(
            pair_rows.at[pl.ds(beside(d) * 16 + n * 4, 4), :, half * 128 : half * 128 + 128],
            x.at[half, n * 4 : n * 4 + 4, mine, :],
            row_send, row_recv.at[half, n], device_id={"gz": beside(d)}, device_id_type=MESH,
        )

    def bytes_of(ref, send, recv):
        return pltpu.make_async_remote_copy(ref, ref, send, recv, device_id=other, device_id_type=MESH)

    for d in (1, 3, 2):
        weight_copy(d).start()
    for half in range(2):
        for n in range(4):
            for d in (1, 3, 2):
                row_copy(d, half, n).start()
    for d in (1, 3, 2):
        gain_copy(d).start()
    along_y(near)
    for half in range(2):
        x[half, :, mine, :] = pair_rows[pl.ds(gz * 16, 16), :, half * 128 : half * 128 + 128]
    pl.semaphore_wait(near, 3)
    along_z(far)
    weights_in = bytes_of(weights.at[:, 0:96, :], weight_send, weight_recv)
    weights_in.wait_recv()

    def head_copy(i, half):
        px, py, pz = chip(i)
        return pltpu.make_async_remote_copy(
            to_heads.at[half, (px * 4 + py) * 8 + pz], head_place(half),
            head_send, head_recv.at[half], device_id=device(px, py, pz), device_id_type=MESH,
        )

    def head_place(half):
        rows = pl.ds(pl.multiple_of(gz * 16, 16), 16)
        return held.at[half, :, z, core, rows, pl.ds(pl.multiple_of(gx * 128, 128), 128)]

    for half in range(2):
        for n in range(4):
            bytes_of(pair_rows.at[0:12, :, 0:128], row_send, row_recv.at[half, n]).wait_recv()

            def rows(r, carry):
                i = n * 4 + 2 * r
                values = jnp.concatenate([x[half, i], x[half, i + 1]], axis=1).astype(F32)
                average = jnp.mean(values, axis=0, keepdims=True)
                centered = values - average
                spread = jnp.mean(jnp.square(centered), axis=0, keepdims=True)
                normed = (centered * lax.rsqrt(spread + epsilon) * gain[...]).astype(BF16)
                x[half, i] = normed[:, :128]
                x[half, i + 1] = normed[:, 128:]
                keep = mask[half, n * 2 + r]
                for side in range(2):
                    both = jnp.dot(
                        weights[2 * side : 2 * side + 2].reshape(256, 128), normed,
                        preferred_element_type=F32,
                    )
                    rows_of_side = keep * jax.nn.sigmoid(both[:128]) * both[128:]
                    staged[side, i] = rows_of_side[:, :128]
                    staged[side, i + 1] = rows_of_side[:, 128:]
                return carry

            lax.fori_loop(0, 2, rows, 0)
        for side in range(2):
            for h0 in range(0, 128, 8):
                to_heads[half, h0 : h0 + 8, side] = jnp.swapaxes(
                    staged[side, :, h0 : h0 + 8, :], 0, 1
                ).astype(BF16)
        if half == 0:
            pl.semaphore_wait(far, 7)

        def send_head(i, carry):
            head_copy(i, half).start()
            return carry

        lax.fori_loop(1, 128, send_head, 0)
        head_place(half)[...] = to_heads[half, head]

    def gate_rows(p, carry):
        for half in range(2):
            normed = jnp.concatenate([x[half, 2 * p], x[half, 2 * p + 1]], axis=1)
            gate[half, p] = jax.nn.sigmoid(
                jnp.dot(weights[4], normed, preferred_element_type=F32)
            )
        return carry

    lax.fori_loop(0, 8, gate_rows, 0)

    def core_copy(half, whose):
        part = held.at[half, 1, :, whose]
        return pltpu.make_async_remote_copy(
            part, part, core_send.at[half], core_recv.at[half], device_id=other, device_id_type=MESH
        )

    def multiply(half, side, block):
        left = held[half, 0, :, core].reshape(512, 512)
        right = [held[half, 1, 4 * block + 2 * e + side].reshape(128, 512) for e in range(2)]
        return lax.dot_general(
            left, jnp.concatenate(right, axis=0), (((1,), (1,)), ((), ())),
            preferred_element_type=F32,
        )

    def mix_copy(i, side):
        px, py, pz = chip(i)
        return pltpu.make_async_remote_copy(
            product.at[side, py, pl.ds(pl.multiple_of(pz * 64 + px * 16, 16), 16), :],
            mixed.at[side, head],
            mix_send, mix_recv.at[side], device_id=device(px, py, pz), device_id_type=MESH,
        )

    for half in range(2):
        bytes_of(to_heads.at[half, 0:127], head_send, head_recv.at[half]).wait_recv()
        core_copy(half, core).start()
        core_copy(half, 1 - core).wait_recv()
        for side in range(2):
            for block in range(2):
                if half == 0:
                    total[side, block] = multiply(0, side, block)
                else:
                    summed = (total[side, block] + multiply(1, side, block)).astype(BF16)
                    product[side, 2 * block] = summed[:, :128]
                    product[side, 2 * block + 1] = summed[:, 128:]
            if half == 1:

                def send_mix(i, carry):
                    mix_copy(i, side).start()
                    return carry

                lax.fori_loop(1, 128, send_mix, 0)
                mixed[side, head] = product[
                    side, gx, pl.ds(pl.multiple_of(z * 64 + gz * 16, 16), 16), :
                ]
    bytes_of(out_gain.at[0:96, :], gain_send, gain_recv).wait_recv()

    def up_copy(d, side, n):
        theirs = pl.ds(pl.multiple_of(beside(d) * 32, 32), 32)
        return pltpu.make_async_remote_copy(
            update.at[side, n * 4 : n * 4 + 4, theirs, :],
            out_ref.at[pl.ds(gz * 16 + n * 4, 4), :, side * 128 : side * 128 + 128],
            up_send, up_recv, device_id={"gz": beside(d)}, device_id_type=MESH,
        )

    def own_copy(side):
        return pltpu.make_async_copy(
            update.at[side, :, mine, :],
            out_ref.at[pl.ds(gz * 16, 16), :, side * 128 : side * 128 + 128],
            own.at[side],
        )

    for side in range(2):
        bytes_of(mixed.at[side, 0:127], mix_send, mix_recv.at[side]).wait_recv()
        for h0 in range(0, 128, 8):
            staged[0, :, h0 : h0 + 8, :] = jnp.swapaxes(mixed[side, h0 : h0 + 8].astype(F32), 0, 1)
        for n in range(4):

            def last(r, carry):
                p = n * 2 + r
                values = jnp.concatenate([staged[0, 2 * p], staged[0, 2 * p + 1]], axis=1)
                average = jnp.mean(values, axis=0, keepdims=True)
                centered = values - average
                spread = jnp.mean(jnp.square(centered), axis=0, keepdims=True)
                scale = jnp.concatenate([out_gain[...], out_gain[...]], axis=1)
                normed = (centered * lax.rsqrt(spread + epsilon) * scale).astype(BF16)
                projected = jnp.dot(weights[5], normed, preferred_element_type=F32)
                gated = (gate[side, p] * projected).astype(BF16)
                update[side, 2 * p] = gated[:, :128]
                update[side, 2 * p + 1] = gated[:, 128:]
                return carry

            lax.fori_loop(0, 2, last, 0)
            for d in (1, 3, 2):
                up_copy(d, side, n).start()
        own_copy(side).start()
    bytes_of(out_ref.at[0:48], up_send, up_recv).wait_recv()

    weights_in.wait_send()
    bytes_of(out_gain.at[0:96, :], gain_send, gain_recv).wait_send()
    bytes_of(pair_rows.at[0:48], row_send, row_recv.at[0, 0]).wait_send()
    for half in range(2):
        bytes_of(to_heads.at[half, 0:127], head_send, head_recv.at[0]).wait_send()
        bytes_of(mixed.at[half, 0:127], mix_send, mix_recv.at[0]).wait_send()
        core_copy(half, core).wait_send()
        own_copy(half).wait()
    bytes_of(out_ref.at[0:48], up_send, up_recv).wait_send()


def local(
    pair,
    pair_mask,
    in_gain,
    w_left,
    w_left_gate,
    w_right,
    w_right_gate,
    w_out_gate,
    out_gain,
    w_out,
):
    anywhere = pl.BlockSpec(memory_space=pl.ANY)
    dma, vmem = pltpu.SemaphoreType.DMA, pltpu.VMEM
    rows = pl.pallas_call(
        kernel,
        out_shape=jax.ShapeDtypeStruct((64, 32, 256), BF16),
        in_specs=[anywhere] * 10,
        out_specs=anywhere,
        scratch_shapes=[
            vmem((32, 64, 256), BF16),
            vmem((16, 256), jnp.int32),
            vmem((1, 128), F32),
            vmem((1, 32), F32),
            vmem((6, 32, 128), BF16),
            vmem((64, 32, 256), BF16),
            vmem((2, 16, 128, 128), BF16),
            vmem((6, 128, 128), BF16),
            vmem((128, 256), F32),
            vmem((128, 128), F32),
            vmem((2, 8, 1, 256), F32),
            vmem((2, 16, 128, 128), F32),
            vmem((2, 128, 2, 16, 128), BF16),
            vmem((2, 8, 128, 256), F32),
            vmem((2, 2, 8, 2, 64, 512), BF16),
            vmem((2, 2, 512, 256), F32),
            vmem((2, 4, 512, 128), BF16),
            vmem((2, 128, 16, 128), BF16),
            vmem((2, 16, 128, 128), BF16),
            dma((10,)), pltpu.SemaphoreType.REGULAR, pltpu.SemaphoreType.REGULAR,
            dma, dma((2, 4)), dma, dma, dma, dma,
            dma, dma((2,)), dma((2,)), dma((2,)), dma, dma((2,)), dma, dma, dma((2,)),
        ],
        compiler_params=pltpu.CompilerParams(
            collective_id=0, has_side_effects=True, vmem_limit_bytes=67_043_328
        ),
        name="triangle",
    )(
        pair, pair_mask, in_gain.reshape(1, 128), out_gain.reshape(1, 32),
        w_left_gate.T, w_left.T, w_right_gate.T, w_right.T, w_out_gate.T, w_out.T,
    )
    return jnp.swapaxes(rows, 0, 1)


def solution(mesh):
    placed = (
        P("gz", "gy", "gx"),
        P("gy", "gx"),
        P(),
        P(None, "gz"),
        P(None, "gz"),
        P(None, "gz"),
        P(None, "gz"),
        P(None, "gz"),
        P("gz"),
        P(None, "gz"),
    )
    return jax.shard_map(
        local, mesh=mesh, in_specs=placed, out_specs=P("gz", "gy", "gx"), check_vma=False
    )
```
